256 devices in a mesh: grp: 2 (over y), blk: 16 (over z), node: 4 (over x), pair: 2 (over core).
Axes of the slice: x: 4, y: 2, z: 16, core: 2. Of those that a mesh axis runs over, the one named last changes fastest.
The devices are a block of a 4x16x16 slice.
Arguments:
- query: bfloat16 [18432, 1280], P(('grp', 'blk', 'node'), 'pair'), parts along dimension 0, may hold values from -600 to 600
- key: bfloat16 [18432, 1280], P(('grp', 'blk', 'node'), 'pair'), parts along dimension 0, may hold values from -25 to 25
- value: bfloat16 [18432, 1280], P(('grp', 'blk', 'node'), 'pair'), parts along dimension 0, may hold values from -6 to 6
- out_weight: bfloat16 [1280, 1280], P('pair'), may hold values from -0.15625 to 0.15625
Outputs:
- mixed: bfloat16 [18432, 1280], P(('grp', 'blk', 'node', 'pair')), parts along dimension 0
The draws below stay inside these ranges and needn't reach their ends.
There are 2 independent parts, one for each index of `grp`. The reference program is written for one: setup_inputs(seed, part) draws one part's arguments, and reference() takes and returns one part's arrays. A program takes and returns all parts, laid end to end along the dimension named above; an argument that names none is the same for every part. Nothing has to cross between parts.
All inputs are finite; a program needn't handle non-finite values.
Results may differ from the reference program's by a relative error of at most 0.011.
Values may be sent and summed in bfloat16 or wider, within the bound.
No kernel may reach another device: no remote copies, remote signals or barrier semaphores. Data moves between devices by JAX's collectives and lax.ppermute only.
A program may use at most 128 MiB of HBM per device.

```python
import math
import jax
import jax.numpy as jnp
from jax import lax

D = 1280
HEADS = 20
HD = 64
TOKENS = 9216


def key_rows(key):
    base = jnp.clip(jax.random.normal(jax.random.fold_in(key, 101), (TOKENS, D), jnp.float32), -4.5, 4.5)
    return base.astype(jnp.bfloat16)


def draw_key(key, part):
    return key_rows(key)


def draw_query(key, part):
    drawn = jax.random.normal(jax.random.fold_in(key, 105), (TOKENS, D), jnp.float32) * 2.5
    return jnp.clip(drawn, -12.0, 12.0).astype(jnp.bfloat16)


def block_levels(own_key, extent, shards, least, top_value):
    gain = 1.0
    for dim, shards_of in shards:
        steps = jax.random.uniform(jax.random.fold_in(jax.random.fold_in(own_key, 6), dim), (shards_of,), jnp.float32, least / len(shards), top_value / len(shards))
        gain = gain * jnp.repeat(jnp.exp(steps), extent[dim] // shards_of).reshape((-1,) + (1,) * (len(extent) - 1 - dim))
    return gain


def scatter_about(rng, shape, scale, reach, cuts=(), held_as=jnp.bfloat16):
    array = scale * jax.random.normal(rng, shape, jnp.float32)
    if cuts:
        array = array * block_levels(rng, shape, cuts, -0.22, 0.18)
    return jnp.clip(array, -reach, reach).astype(held_as)


def setup_inputs(seed: int = 0, part: int = 0) -> dict:
    keys = jax.random.split(jax.random.key(seed), 5)
    own_keys = jax.random.split(jax.random.fold_in(keys[4], part), 5)
    return {
        "query": draw_query(jax.random.fold_in(jax.random.fold_in(keys[4], part), 71), part),
        "key": draw_key(jax.random.fold_in(jax.random.fold_in(keys[4], part), 71), part),
        "value": scatter_about(own_keys[2], (TOKENS, D), 1.0, 6.0, ((0, 64), (1, 2))),
        "out_weight": scatter_about(keys[3], (D, D), D ** -0.5, 0.15625, ((0, 2),)),
    }


def reference(query, key, value, out_weight):
    scale = 1.0 / math.sqrt(HD)
    q_heads = query.reshape(TOKENS, HEADS, HD).transpose(1, 0, 2)
    k_heads = key.reshape(TOKENS, HEADS, HD).transpose(1, 0, 2)
    v_heads = value.reshape(TOKENS, HEADS, HD).transpose(1, 0, 2)

    def one_head(operands):
        q_one, k_one, v_one = operands
        scores = jnp.dot(q_one, k_one.T, preferred_element_type=jnp.float32) * scale
        peak = lax.optimization_barrier(jnp.max(scores, axis=1, keepdims=True))
        expo = jnp.exp(scores - peak)
        total = lax.optimization_barrier(jnp.sum(expo, axis=1, keepdims=True))
        return jnp.dot(expo.astype(jnp.bfloat16), v_one, preferred_element_type=jnp.float32) / total
    heads_out = lax.map(one_head, (q_heads, k_heads, v_heads))
    attn = heads_out.transpose(1, 0, 2).reshape(TOKENS, D).astype(jnp.bfloat16)
    return jnp.dot(attn, out_weight, preferred_element_type=jnp.float32).astype(jnp.bfloat16)
```

```python
import math

import jax
import jax.numpy as jnp
from jax import lax
from jax.experimental import pallas as pl
from jax.experimental.pallas import tpu as pltpu
from jax.sharding import PartitionSpec as P

HD = 64
LANES = 128
LOWEST = -1e30


def round_up(value, unit):
    return -(-value // unit) * unit


def shifted(array, axis, by):
    size = lax.axis_size(axis)
    return lax.ppermute(array, axis, [(i, (i + by) % size) for i in range(size)])


def split_three(x):
    hi = x.astype(jnp.bfloat16).astype(jnp.float32)
    rest = x - hi
    mid = rest.astype(jnp.bfloat16).astype(jnp.float32)
    return hi, mid, rest - mid


def attend_step(queries, keys, values, state, last):
    count, features = queries.shape
    pairs = features // LANES
    heads = features // HD
    hrows = round_up(heads, 8)
    pieces = len(keys)
    factor = (1.0 / math.sqrt(HD)) * math.log2(math.e)
    fresh_state = state is None

    def body(*refs):
        q_ref = refs[0]
        k_refs = refs[1 : 1 + pieces]
        v_refs = refs[1 + pieces : 1 + 2 * pieces]
        at = 1 + 2 * pieces
        if not fresh_state:
            m_in, l_in, a_in = refs[at : at + 3]
            at += 3
        if last:
            o_ref, m_out, l_out = refs[at : at + 3]
        else:
            m_out, l_out, a_out = refs[at : at + 3]

        def pair_step(p, carry):
            lanes = pl.ds(pl.multiple_of(p * LANES, LANES), LANES)
            kk = jnp.concatenate([r[:, lanes] for r in k_refs], axis=0)
            vv = jnp.concatenate([r[:, lanes] for r in v_refs], axis=0)
            vt = vv.T
            qq = q_ref[:, lanes]
            lane = lax.broadcasted_iota(jnp.int32, qq.shape, 1)
            ones = jnp.ones((16, vt.shape[1]), vt.dtype)
            outs = []
            for side in range(2):
                row = pl.ds(2 * p + side, 1)
                mask = (lane < HD) if side == 0 else (lane >= HD)
                qm = jnp.where(mask, qq, jnp.zeros_like(qq))
                s = lax.dot_general(
                    kk, qm, (((1,), (1,)), ((), ())), preferred_element_type=jnp.float32
                )
                peak = jnp.max(s, axis=0, keepdims=True)
                if not fresh_state:
                    old = m_in[row, :]
                    peak = jnp.maximum(old, peak)
                expo = jnp.exp2((s - peak) * factor).astype(jnp.bfloat16)
                vs = jnp.concatenate([vt[side * HD : (side + 1) * HD, :], ones], axis=0)
                pv = jnp.dot(vs, expo, preferred_element_type=jnp.float32)
                acc = pv[:HD, :]
                total = pv[HD : HD + 1, :]
                arows = pl.ds(pl.multiple_of(p * LANES + side * HD, HD), HD)
                if not fresh_state:
                    fade = jnp.exp2((old - peak) * factor)
                    acc = a_in[arows, :] * fade + acc
                    total = l_in[row, :] * fade + total
                m_out[row, :] = peak
                l_out[row, :] = total
                if last:
                    outs.append(acc / total)
                else:
                    a_out[arows, :] = acc
            if last:
                both = jnp.concatenate(outs, axis=0)
                o_ref[:, lanes] = both.T.astype(jnp.bfloat16)
            return carry

        lax.fori_loop(0, pairs, pair_step, 0)
        if last:
            live = lax.broadcasted_iota(jnp.int32, m_out.shape, 0) < heads
            parts = split_three(jnp.where(live, m_out[...], 0.0))
            parts += split_three(jnp.where(live, l_out[...], 1.0))
            parts += (jnp.zeros((LANES - 6 * hrows, count), jnp.float32),)
            o_ref[:, features:] = jnp.concatenate(parts, axis=0).T.astype(jnp.bfloat16)

    stat = jax.ShapeDtypeStruct((hrows, count), jnp.float32)
    args = [queries, *keys, *values]
    aliases = {}
    if not fresh_state:
        first = len(args)
        args += list(state)
    if last:
        outs = (jax.ShapeDtypeStruct((count, features + LANES), jnp.bfloat16), stat, stat)
    else:
        outs = (stat, stat, jax.ShapeDtypeStruct((features, count), jnp.float32))
        if not fresh_state:
            aliases = {first: 0, first + 1: 1, first + 2: 2}
    rows = sum(k.shape[0] for k in keys)
    vmem = pl.BlockSpec(memory_space=pltpu.VMEM)
    return pl.pallas_call(
        body,
        out_shape=outs,
        in_specs=[vmem] * len(args),
        out_specs=tuple([vmem] * 3),
        input_output_aliases=aliases,
        cost_estimate=pl.CostEstimate(
            flops=4 * rows * count * features,
            transcendentals=rows * count * heads,
            bytes_accessed=4 * count * features,
        ),
        compiler_params=pltpu.CompilerParams(vmem_limit_bytes=40 * 2**20),
        name="attend",
    )(*args)


def merge_project(parts, weight):
    items, wide = parts[0].shape
    features = wide - LANES
    heads = features // HD
    hrows = round_up(heads, 8)
    width = weight.shape[1]

    def body(*refs):
        p_refs, w_ref, o_ref = refs[:-2], refs[-2], refs[-1]
        stats = [r[:, features:].astype(jnp.float32) for r in p_refs]

        def stat(x, which):
            at = 3 * which * hrows
            return (
                x[:, at : at + hrows]
                + x[:, at + hrows : at + 2 * hrows]
                + x[:, at + 2 * hrows : at + 3 * hrows]
            )

        peaks = [stat(x, 0) for x in stats]
        best = peaks[0]
        for m in peaks[1:]:
            best = jnp.maximum(best, m)
        factor = (1.0 / math.sqrt(HD)) * math.log2(math.e)
        shares = [jnp.exp2((m - best) * factor) * stat(x, 1) for m, x in zip(peaks, stats)]
        total = shares[0]
        for w in shares[1:]:
            total = total + w
        shares = [w / total for w in shares]
        lane = lax.broadcasted_iota(jnp.int32, (items, LANES), 1)
        out = jnp.zeros((items, width), jnp.float32)
        columns = []
        for p in range(features // LANES):
            joined = jnp.zeros((items, LANES), jnp.float32)
            for r, w in zip(p_refs, shares):
                scale = jnp.where(lane < HD, w[:, 2 * p : 2 * p + 1], w[:, 2 * p + 1 : 2 * p + 2])
                joined += r[:, p * LANES : (p + 1) * LANES].astype(jnp.float32) * scale
            columns.append(joined.astype(jnp.bfloat16))
        attn = jnp.concatenate(columns, axis=1)
        out = jnp.dot(attn, w_ref[...], preferred_element_type=jnp.float32)
        o_ref[...] = out.astype(jnp.bfloat16)

    vmem = pl.BlockSpec(memory_space=pltpu.VMEM)
    return pl.pallas_call(
        body,
        out_shape=jax.ShapeDtypeStruct((items, width), jnp.bfloat16),
        in_specs=[vmem] * (len(parts) + 1),
        out_specs=vmem,
        cost_estimate=pl.CostEstimate(
            flops=2 * items * features * width, transcendentals=0, bytes_accessed=2 * features * width
        ),
        compiler_params=pltpu.CompilerParams(vmem_limit_bytes=40 * 2**20),
        name="merge_project",
    )(*parts, weight)


def per_device(query, key, value, out_weight):
    rows, features = query.shape
    blks = lax.axis_size("blk")
    nodes = lax.axis_size("node")
    half = blks // 2

    turns = sorted(range(1, nodes), key=lambda d: -min(d, nodes - d))
    others = {d: shifted(query, "node", d) for d in turns}
    pieces = [query] + [others[d] for d in range(1, nodes)]
    count = rows * nodes
    padded = round_up(count, LANES)
    if padded > count:
        pieces.append(jnp.zeros((padded - count, features), query.dtype))
    queries = jnp.concatenate(pieces, axis=0)

    k_up, v_up, k_down, v_down = key, value, key, value
    state = None
    held_k, held_v = [key], [value]
    done = queries
    for turn in range(1, half + 1):
        final = turn == half
        if turn > 1:
            k_up, k_down, done = lax.optimization_barrier((k_up, k_down, done))
            v_up, v_down, _ = lax.optimization_barrier((v_up, v_down, done))
            if turn == 2:
                queries = done
            else:
                state = (done,) + state[1:]
        next_k_up = shifted(k_up, "blk", 1)
        next_v_down = shifted(v_down, "blk", -1)
        if not final:
            next_k_down = shifted(k_down, "blk", -1)
            next_v_up = shifted(v_up, "blk", 1)
        if turn > 1:
            state = attend_step(queries, held_k, held_v, state, False)
            done = state[0]
            held_k, held_v = [], []
        k_up, v_down = next_k_up, next_v_down
        held_k.append(k_up)
        if not final:
            k_down, v_up = next_k_down, next_v_up
            held_k.append(k_down)
            held_v.append(v_up)
        held_v.append(v_down)
    state = attend_step(queries, held_k, held_v, state, True)

    partial = state[0]
    blocks = [partial[i * rows : (i + 1) * rows] for i in range(nodes)]
    back = {d: shifted(blocks[d], "node", -d) for d in turns}
    parts = [blocks[0]] + [back[d] for d in range(1, nodes)]
    mine = merge_project(parts, out_weight)

    pairs = lax.axis_size("pair")
    at = lax.axis_index("pair")
    tiles = mine.reshape(pairs, rows // pairs, mine.shape[1])
    summed = lax.dynamic_index_in_dim(tiles, at, 0, keepdims=False).astype(jnp.float32)
    for d in range(1, pairs):
        sent = lax.dynamic_index_in_dim(tiles, (at + d) % pairs, 0, keepdims=False)
        summed = summed + shifted(sent, "pair", d).astype(jnp.float32)
    return summed.astype(jnp.bfloat16)


def solution(mesh):
    in_specs = (
        P(("grp", "blk", "node"), "pair"),
        P(("grp", "blk", "node"), "pair"),
        P(("grp", "blk", "node"), "pair"),
        P("pair", None),
    )
    out_specs = P(("grp", "blk", "node", "pair"), None)
    return jax.shard_map(
        per_device, mesh=mesh, in_specs=in_specs, out_specs=out_specs, check_vma=False
    )
```

```python
import math

import jax
import jax.numpy as jnp
from jax import lax
from jax.experimental import pallas as pl
from jax.experimental.pallas import tpu as pltpu
from jax.sharding import PartitionSpec as P


HD = 64
LANES = 128


def round_up(value, unit):
    return -(-value // unit) * unit


def shifted(array, axis, by):
    size = lax.axis_size(axis)
    return lax.ppermute(array, axis, [(i, (i + by) % size) for i in range(size)])


def split_three(x):
    hi = x.astype(jnp.bfloat16).astype(jnp.float32)
    rest = x - hi
    mid = rest.astype(jnp.bfloat16).astype(jnp.float32)
    return hi, mid, rest - mid


def attend_step(queries, pieces, state, offset, pairs, last, other=None):
    count = queries.shape[0]
    features = pairs * LANES
    heads = features // HD
    hrows = round_up(heads, 8)
    factor = (1.0 / math.sqrt(HD)) * math.log2(math.e)
    fresh_state = state is None

    args = [queries]
    spots = []
    for k, k_at, v, v_at in pieces:
        args.append(k)
        spots.append((len(args) - 1, k_at, len(args) - 1 if v is k else len(args), v_at))
        if v is not k:
            args.append(v)
    first = len(args)
    if not fresh_state:
        args += list(state)
    if other is not None:
        args += [other[0], other[1]]
    inputs = len(args)

    def body(*refs):
        q_ref = refs[0]
        if not fresh_state:
            m_in, l_in, a_in = refs[first : first + 3]
        if last:
            o_ref, m_out, l_out = refs[inputs : inputs + 3]
        else:
            m_out, l_out, a_out = refs[inputs : inputs + 3]
        s_ref = refs[-1]

        def lanes_of(p, start):
            return pl.ds(pl.multiple_of(start + p * LANES, LANES), LANES)

        def score(p, side):
            kk = jnp.concatenate([refs[i][:, lanes_of(p, at)] for i, at, _, _ in spots], axis=0)
            qq = q_ref[:, lanes_of(p, offset)]
            lane = lax.broadcasted_iota(jnp.int32, qq.shape, 1)
            mask = (lane < HD) if side == 0 else (lane >= HD)
            qm = jnp.where(mask, qq, jnp.zeros_like(qq))
            return lax.dot_general(
                kk, qm, (((1,), (1,)), ((), ())), preferred_element_type=jnp.float32
            )

        def finish(p, side, s, vt):
            row = pl.ds(2 * p + side, 1)
            peak = jnp.max(s, axis=0, keepdims=True)
            if not fresh_state:
                old = m_in[row, :]
                peak = jnp.maximum(old, peak)
            expo = jnp.exp2((s - peak) * factor).astype(jnp.bfloat16)
            ones = jnp.ones((16, vt.shape[1]), vt.dtype)
            vs = jnp.concatenate([vt[side * HD : (side + 1) * HD, :], ones], axis=0)
            pv = jnp.dot(vs, expo, preferred_element_type=jnp.float32)
            acc = pv[:HD, :]
            total = pv[HD : HD + 1, :]
            arows = pl.ds(pl.multiple_of(p * LANES + side * HD, HD), HD)
            if not fresh_state:
                fade = jnp.exp2((old - peak) * factor)
                acc = a_in[arows, :] * fade + acc
                total = l_in[row, :] * fade + total
            m_out[row, :] = peak
            l_out[row, :] = total
            if last:
                return acc / total
            a_out[arows, :] = acc
            return None

        def pair_step(p, carry):
            vt = jnp.concatenate([refs[i][:, lanes_of(p, at)] for _, _, i, at in spots], axis=0).T
            later = score(p, 1)
            first_out = finish(p, 0, s_ref[0], vt)
            s_ref[1] = later
            ahead = score(jnp.minimum(p + 1, pairs - 1), 0)
            second_out = finish(p, 1, s_ref[1], vt)
            s_ref[0] = ahead
            if last:
                both = jnp.concatenate([first_out, second_out], axis=0)
                o_ref[:, lanes_of(p, 0)] = both.T.astype(jnp.bfloat16)
            return carry

        s_ref[0] = score(0, 0)
        lax.fori_loop(0, pairs, pair_step, 0)
        if other is not None:
            o_m, o_l = refs[inputs - 2 : inputs]
            live = lax.broadcasted_iota(jnp.int32, m_out.shape, 0) < heads
            parts = []
            for theirs, ours in ((o_m, m_out), (o_l, l_out)):
                both = jnp.concatenate([theirs[...], jnp.where(live, ours[...], 1.0)], axis=0)
                parts += list(split_three(both))
            used = sum(p.shape[0] for p in parts)
            parts.append(jnp.zeros((LANES - used, count), jnp.float32))
            o_ref[:, features:] = jnp.concatenate(parts, axis=0).T.astype(jnp.bfloat16)
        elif last:
            dead = lax.broadcasted_iota(jnp.int32, m_out.shape, 0) >= heads
            m_out[...] = jnp.where(dead, 1.0, m_out[...])
            l_out[...] = jnp.where(dead, 1.0, l_out[...])

    stat = jax.ShapeDtypeStruct((hrows, count), jnp.float32)
    aliases = {}
    if last:
        wide = features if other is None else features + LANES
        outs = (jax.ShapeDtypeStruct((count, wide), jnp.bfloat16), stat, stat)
    else:
        outs = (stat, stat, jax.ShapeDtypeStruct((features, count), jnp.float32))
        if not fresh_state:
            aliases = {first: 0, first + 1: 1, first + 2: 2}
    rows = sum(p[0].shape[0] for p in pieces)
    vmem = pl.BlockSpec(memory_space=pltpu.VMEM)
    return pl.pallas_call(
        body,
        out_shape=outs,
        in_specs=[vmem] * inputs,
        out_specs=(vmem, vmem, vmem),
        input_output_aliases=aliases,
        scratch_shapes=[pltpu.VMEM((2, rows, count), jnp.float32)],
        cost_estimate=pl.CostEstimate(
            flops=4 * rows * count * features,
            transcendentals=rows * count * heads,
            bytes_accessed=4 * count * features,
        ),
        compiler_params=pltpu.CompilerParams(vmem_limit_bytes=40 * 2**20),
        name="attend",
    )(*args)


def merge_project(groups, weight):
    items = groups[0][0].shape[0]
    width = weight.shape[1]
    sources = len(groups[0])
    factor = (1.0 / math.sqrt(HD)) * math.log2(math.e)
    wides = [g[0].shape[1] for g in groups]
    wides[-1] -= LANES
    starts = [0]
    for w in wides:
        starts.append(starts[-1] + round_up(w // HD, 8))
    hrows = starts[-1]

    def body(*refs):
        w_ref, o_ref = refs[-2], refs[-1]
        tails = refs[(len(groups) - 1) * sources : len(groups) * sources]
        stats = [r[:, wides[-1] :].astype(jnp.float32) for r in tails]

        def stat(x, which):
            at = 3 * which * hrows
            return (
                x[:, at : at + hrows]
                + x[:, at + hrows : at + 2 * hrows]
                + x[:, at + 2 * hrows : at + 3 * hrows]
            )

        peaks = [stat(x, 0) for x in stats]
        best = peaks[0]
        for m in peaks[1:]:
            best = jnp.maximum(best, m)
        shares = [jnp.exp2((m - best) * factor) * stat(x, 1) for m, x in zip(peaks, stats)]
        total = shares[0]
        for w in shares[1:]:
            total = total + w
        shares = [w / total for w in shares]
        lane = lax.broadcasted_iota(jnp.int32, (items, LANES), 1)
        columns = []
        for g, wide in enumerate(wides):
            for p in range(wide // LANES):
                joined = jnp.zeros((items, LANES), jnp.float32)
                at = starts[g] + 2 * p
                for r, w in zip(refs[g * sources : (g + 1) * sources], shares):
                    scale = jnp.where(lane < HD, w[:, at : at + 1], w[:, at + 1 : at + 2])
                    joined += r[:, p * LANES : (p + 1) * LANES].astype(jnp.float32) * scale
                columns.append(joined.astype(jnp.bfloat16))
        attn = jnp.concatenate(columns, axis=1)
        out = jnp.dot(attn, w_ref[...], preferred_element_type=jnp.float32)
        o_ref[...] = out.astype(jnp.bfloat16)

    vmem = pl.BlockSpec(memory_space=pltpu.VMEM)
    parts = [p for g in groups for p in g]
    return pl.pallas_call(
        body,
        out_shape=jax.ShapeDtypeStruct((items, width), jnp.bfloat16),
        in_specs=[vmem] * (len(parts) + 1),
        out_specs=vmem,
        cost_estimate=pl.CostEstimate(
            flops=2 * items * weight.shape[0] * width,
            transcendentals=0,
            bytes_accessed=2 * weight.shape[0] * width,
        ),
        compiler_params=pltpu.CompilerParams(vmem_limit_bytes=40 * 2**20),
        name="merge_project",
    )(*parts, weight)


def per_device(query, key, value, out_weight):
    rows, features = query.shape
    blks = lax.axis_size("blk")
    nodes = lax.axis_size("node")
    half = blks // 2
    pairs = features // LANES
    cut = pairs - pairs // 2
    spans = ((0, cut), (cut, pairs))
    widths = [(p1 - p0) * LANES for p0, p1 in spans]

    def group_of(array, g):
        return array[:, spans[g][0] * LANES : spans[g][1] * LANES]

    own = [jnp.concatenate([group_of(key, g), group_of(value, g)], axis=1) for g in range(2)]
    up, down = list(own), list(own)
    held = [[(own[g], 0, own[g], widths[g])] for g in range(2)]
    states = [None, None]
    gate = None
    turns = sorted(range(1, nodes), key=lambda d: -min(d, nodes - d))
    others = {}
    queries = None
    blocks = [None, None]
    sent = [{}, {}]

    def attend(g, last):
        nonlocal gate
        other = states[0] if last and g == 1 else None
        got = attend_step(
            queries, held[g], states[g], spans[g][0] * LANES, widths[g] // LANES, last, other
        )
        held[g] = []
        if last:
            blocks[g] = [got[0][i * rows : (i + 1) * rows] for i in range(nodes)]
            states[g] = got[1:]
        else:
            states[g] = got
            gate = got[0]

    for turn in range(1, half + 1):
        final = turn == half
        for g in range(2):
            width = widths[g]
            a, b = up[g], down[g]
            if gate is not None:
                a, b, gate = lax.optimization_barrier((a, b, gate))
            if final:
                k = shifted(a[:, :width], "blk", 1)
                v = shifted(b[:, width:], "blk", -1)
                arrived = [(k, 0, v, 0)]
            else:
                up[g] = shifted(a, "blk", 1)
                down[g] = shifted(b, "blk", -1)
                arrived = [(up[g], 0, up[g], width), (down[g], 0, down[g], width)]
            if turn == 1 and g == 0:
                for d in turns:
                    others[d] = shifted(query, "node", d)
                stack = [query] + [others[d] for d in range(1, nodes)]
                padded = round_up(rows * nodes, LANES)
                if padded > rows * nodes:
                    stack.append(jnp.zeros((padded - rows * nodes, features), query.dtype))
                queries = jnp.concatenate(stack, axis=0)
            if turn > 1:
                attend(g, False)
            held[g] = held[g] + arrived

    for g in range(2):
        attend(g, True)
        sent[g] = {d: shifted(blocks[g][d], "node", -d) for d in turns}
    groups = [[blocks[g][0]] + [sent[g][d] for d in range(1, nodes)] for g in range(2)]
    mine = merge_project(groups, out_weight)

    cores = lax.axis_size("pair")
    at = lax.axis_index("pair")
    tiles = mine.reshape(cores, rows // cores, mine.shape[1])
    summed = lax.dynamic_index_in_dim(tiles, at, 0, keepdims=False).astype(jnp.float32)
    for d in range(1, cores):
        away = lax.dynamic_index_in_dim(tiles, (at + d) % cores, 0, keepdims=False)
        summed = summed + shifted(away, "pair", d).astype(jnp.float32)
    return summed.astype(jnp.bfloat16)


def solution(mesh):
    in_specs = (
        P(("grp", "blk", "node"), "pair"),
        P(("grp", "blk", "node"), "pair"),
        P(("grp", "blk", "node"), "pair"),
        P("pair", None),
    )
    out_specs = P(("grp", "blk", "node", "pair"), None)

    return jax.shard_map(
        per_device, mesh=mesh, in_specs=in_specs, out_specs=out_specs, check_vma=False
    )
```

```python
import math

import jax
import jax.numpy as jnp
from jax import lax
from jax.experimental import pallas as pl
from jax.experimental.pallas import tpu as pltpu
from jax.sharding import PartitionSpec as P


HD = 64
LANES = 128


def round_up(value, unit):
    return -(-value // unit) * unit


def shifted(array, axis, by):
    size = lax.axis_size(axis)
    return lax.ppermute(array, axis, [(i, (i + by) % size) for i in range(size)])


def split_three(x):
    hi = x.astype(jnp.bfloat16).astype(jnp.float32)
    rest = x - hi
    mid = rest.astype(jnp.bfloat16).astype(jnp.float32)
    return hi, mid, rest - mid


def attend_step(queries, pieces, state, last, blocks=None):
    count, features = queries.shape
    pairs = features // LANES
    heads = features // HD
    hrows = round_up(heads + 1, 8)
    factor = (1.0 / math.sqrt(HD)) * math.log2(math.e)
    fresh_state = state is None

    args = [queries]
    spots = []
    for k, k_at, v, v_at, size in pieces:
        args.append(k)
        at = len(args) - 1
        if v is not k:
            args.append(v)
        spots.append((at, slice(k_at, k_at + size), len(args) - 1, slice(v_at, v_at + size)))
    first = len(args)
    if not fresh_state:
        args += list(state)
    inputs = len(args)
    rows = sum(p[4] for p in pieces)
    outputs = 3 if not last else 2 + len(blocks)

    def body(*refs):
        q_ref = refs[0]
        if not fresh_state:
            m_in, l_in, a_in = refs[first : first + 3]
        outs = refs[inputs : inputs + outputs]
        m_out, l_out = outs[:2]
        s0_ref, s1_ref, p0_ref, p1_ref, vt_ref, fade_ref = refs[inputs + outputs :][:6]
        a_out = refs[-1] if last else outs[2]

        def lanes_of(p):
            return pl.ds(pl.multiple_of(p * LANES, LANES), LANES)

        def score(p, side):
            kk = jnp.concatenate([refs[i][at, lanes_of(p)] for i, at, _, _ in spots], axis=0)
            qq = q_ref[:, lanes_of(p)]
            lane = lax.broadcasted_iota(jnp.int32, qq.shape, 1)
            mine = (lane < HD) if side == 0 else (lane >= HD)
            qm = jnp.where(mine, qq, jnp.zeros_like(qq))
            return lax.dot_general(
                kk, qm, (((1,), (1,)), ((), ())), preferred_element_type=jnp.float32
            )

        def softmax(h, s_ref, p_ref):
            row = pl.ds(h, 1)
            peak = s_ref[0:8, :]
            for at in range(8, rows, 8):
                peak = jnp.maximum(peak, s_ref[at : at + 8, :])
            peak = jnp.max(peak, axis=0, keepdims=True)
            if not fresh_state:
                old = m_in[row, :]
                peak = jnp.maximum(old, peak)
                fade_ref[row, :] = jnp.exp2((old - peak) * factor)
            m_out[row, :] = peak
            for at in range(0, rows, 16):
                part = s_ref[at : at + 16, :]
                p_ref[at : at + 16, :] = jnp.exp2((part - peak) * factor).astype(jnp.bfloat16)

        def values(h, expo, vt):
            vs = jnp.concatenate([vt, jnp.ones((16, rows), vt.dtype)], axis=0)
            pv = jnp.dot(vs, expo, preferred_element_type=jnp.float32)
            acc = pv[:HD, :]
            total = pv[HD : HD + 1, :]
            row = pl.ds(h, 1)
            arows = pl.ds(pl.multiple_of(h * HD, HD), HD)
            if not fresh_state:
                fade = fade_ref[row, :]
                acc = a_in[arows, :] * fade + acc
                total = l_in[row, :] * fade + total
            l_out[row, :] = total
            a_out[arows, :] = acc / total if last else acc

        def pair_step(p, carry):
            h = 2 * p
            vv = jnp.concatenate([refs[i][at, lanes_of(p)] for _, _, i, at in spots], axis=0)
            vt = vv.T
            s1_ref[...] = score(p, 1)
            softmax(h, s0_ref, p0_ref)
            values(jnp.where(p == 0, heads, h - 1), p1_ref[...], vt_ref[...])
            s0_ref[...] = score(jnp.minimum(p + 1, pairs - 1), 0)
            softmax(h + 1, s1_ref, p1_ref)
            values(h, p0_ref[...], vt[:HD, :])
            vt_ref[...] = vt[HD:, :]
            return carry

        s0_ref[...] = score(0, 0)
        lax.fori_loop(0, pairs, pair_step, 0)
        values(heads - 1, p1_ref[...], vt_ref[...])
        if last:
            dead = lax.broadcasted_iota(jnp.int32, m_out.shape, 0) >= heads
            m_out[...] = jnp.where(dead, 1.0, m_out[...])
            l_out[...] = jnp.where(dead, 1.0, l_out[...])

            def write(lanes, array):
                at = 0
                for o_ref, size in zip(outs[2:], blocks):
                    o_ref[:, lanes] = array[at : at + size, :]
                    at += size

            for p in range(pairs):
                lanes = slice(p * LANES, (p + 1) * LANES)
                write(lanes, a_out[lanes, :].T.astype(jnp.bfloat16))
            parts = [*split_three(m_out[...]), *split_three(l_out[...])]
            parts.append(jnp.zeros((LANES - 6 * hrows, count), jnp.float32))
            stats = jnp.concatenate(parts, axis=0).T.astype(jnp.bfloat16)
            write(slice(features, features + LANES), stats)

    stat = jax.ShapeDtypeStruct((hrows, count), jnp.float32)
    aliases = {}
    if last:
        wide = features + LANES
        outs = (stat, stat) + tuple(jax.ShapeDtypeStruct((n, wide), jnp.bfloat16) for n in blocks)
    else:
        outs = (stat, stat, jax.ShapeDtypeStruct((features + HD, count), jnp.float32))
        if not fresh_state:
            aliases = {first: 0, first + 1: 1, first + 2: 2}
    scratch = [
        pltpu.VMEM((rows, count), jnp.float32),
        pltpu.VMEM((rows, count), jnp.float32),
        pltpu.VMEM((rows, count), jnp.bfloat16),
        pltpu.VMEM((rows, count), jnp.bfloat16),
        pltpu.VMEM((HD, rows), jnp.bfloat16),
        pltpu.VMEM((hrows, count), jnp.float32),
    ]
    if last:
        scratch.append(pltpu.VMEM((features + HD, count), jnp.float32))
    vmem = pl.BlockSpec(memory_space=pltpu.VMEM)
    return pl.pallas_call(
        body,
        out_shape=outs,
        in_specs=[vmem] * inputs,
        out_specs=tuple([vmem] * outputs),
        input_output_aliases=aliases,
        scratch_shapes=scratch,
        cost_estimate=pl.CostEstimate(
            flops=4 * rows * count * features,
            transcendentals=rows * count * heads,
            bytes_accessed=4 * count * features,
        ),
        compiler_params=pltpu.CompilerParams(vmem_limit_bytes=16 * 2**20),
        name="attend",
    )(*args)


def merge_project(parts, weight):
    items, wide = parts[0].shape
    features = wide - LANES
    heads = features // HD
    hrows = round_up(heads + 1, 8)
    width = weight.shape[1]
    factor = (1.0 / math.sqrt(HD)) * math.log2(math.e)

    def body(*refs):
        w_ref, o_ref = refs[-2], refs[-1]
        stats = [r[:, features:].astype(jnp.float32) for r in refs[:-2]]

        def stat(x, which):
            at = 3 * which * hrows
            return (
                x[:, at : at + hrows]
                + x[:, at + hrows : at + 2 * hrows]
                + x[:, at + 2 * hrows : at + 3 * hrows]
            )

        peaks = [stat(x, 0) for x in stats]
        best = peaks[0]
        for m in peaks[1:]:
            best = jnp.maximum(best, m)
        shares = [jnp.exp2((m - best) * factor) * stat(x, 1) for m, x in zip(peaks, stats)]
        total = shares[0]
        for w in shares[1:]:
            total = total + w
        shares = [w / total for w in shares]
        lane = lax.broadcasted_iota(jnp.int32, (items, LANES), 1)
        columns = []
        for p in range(features // LANES):
            joined = jnp.zeros((items, LANES), jnp.float32)
            for r, w in zip(refs[:-2], shares):
                scale = jnp.where(lane < HD, w[:, 2 * p : 2 * p + 1], w[:, 2 * p + 1 : 2 * p + 2])
                joined += r[:, p * LANES : (p + 1) * LANES].astype(jnp.float32) * scale
            columns.append(joined.astype(jnp.bfloat16))
        attn = jnp.concatenate(columns, axis=1)
        out = jnp.dot(attn, w_ref[...], preferred_element_type=jnp.float32)
        o_ref[...] = out.astype(jnp.bfloat16)

    vmem = pl.BlockSpec(memory_space=pltpu.VMEM)
    return pl.pallas_call(
        body,
        out_shape=jax.ShapeDtypeStruct((items, width), jnp.bfloat16),
        in_specs=[vmem] * (len(parts) + 1),
        out_specs=vmem,
        cost_estimate=pl.CostEstimate(
            flops=2 * items * features * width,
            transcendentals=0,
            bytes_accessed=2 * features * width,
        ),
        compiler_params=pltpu.CompilerParams(vmem_limit_bytes=16 * 2**20),
        name="merge_project",
    )(*parts, weight)


def per_device(query, key, value, out_weight):
    rows, features = query.shape
    blks = lax.axis_size("blk")
    nodes = lax.axis_size("node")
    half = blks // 2

    def piece(both):
        return (both, 0, both, rows, rows)

    own = jnp.concatenate([key, value], axis=0)
    up = down = own
    held = [piece(own)]
    state = None
    for turn in range(1, half + 1):
        final = turn == half
        if final:
            k = shifted(up[:rows], "blk", 1)
            v = shifted(down[rows:], "blk", -1)
            arrived = [(k, 0, v, 0, rows)]
        else:
            up = shifted(up, "blk", 1)
            down = shifted(down, "blk", -1)
            arrived = [piece(up), piece(down)]
        if turn == 1:
            stack = [query] + [shifted(query, "node", d) for d in range(1, nodes)]
            blocks = [rows] * nodes
            padded = round_up(rows * nodes, LANES)
            if padded > rows * nodes:
                stack.append(jnp.zeros((padded - rows * nodes, features), query.dtype))
            queries = jnp.concatenate(stack, axis=0)
        else:
            state = attend_step(queries, held, state, False)
            held = []
        held = held + arrived

    parts = list(attend_step(queries, held, state, True, blocks)[2:])
    for d in range(1, nodes):
        parts[d] = shifted(parts[d], "node", -d)
    mine = merge_project(parts, out_weight)

    cores = lax.axis_size("pair")
    at = lax.axis_index("pair")
    tiles = mine.reshape(cores, rows // cores, mine.shape[1])
    summed = lax.dynamic_index_in_dim(tiles, at, 0, keepdims=False).astype(jnp.float32)
    for d in range(1, cores):
        away = lax.dynamic_index_in_dim(tiles, (at + d) % cores, 0, keepdims=False)
        summed = summed + shifted(away, "pair", d).astype(jnp.float32)
    return summed.astype(jnp.bfloat16)


def solution(mesh):
    in_specs = (
        P(("grp", "blk", "node"), "pair"),
        P(("grp", "blk", "node"), "pair"),
        P(("grp", "blk", "node"), "pair"),
        P("pair", None),
    )
    out_specs = P(("grp", "blk", "node", "pair"), None)

    return jax.shard_map(
        per_device, mesh=mesh, in_specs=in_specs, out_specs=out_specs, check_vma=False
    )
```

```python
import math

import jax
import jax.numpy as jnp
from jax import lax
from jax.experimental import pallas as pl
from jax.experimental.pallas import tpu as pltpu
from jax.sharding import PartitionSpec as P


HD = 64
LANES = 128


def round_up(value, unit):
    return -(-value // unit) * unit


def shifted(array, axis, by):
    size = lax.axis_size(axis)
    return lax.ppermute(array, axis, [(i, (i + by) % size) for i in range(size)])


def split_three(x):
    hi = x.astype(jnp.bfloat16).astype(jnp.float32)
    rest = x - hi
    mid = rest.astype(jnp.bfloat16).astype(jnp.float32)
    return hi, mid, rest - mid


def attend_step(queries, pieces, state, last, blocks=None):
    count, features = queries.shape
    pairs = features // LANES
    heads = features // HD
    hrows = round_up(heads + 1, 8)
    factor = (1.0 / math.sqrt(HD)) * math.log2(math.e)
    fresh_state = state is None

    args = [queries]
    spots = []
    for k, k_at, v, v_at, size in pieces:
        args.append(k)
        at = len(args) - 1
        if v is not k:
            args.append(v)
        spots.append((at, slice(k_at, k_at + size), len(args) - 1, slice(v_at, v_at + size)))
    first = len(args)
    if not fresh_state:
        args += list(state)
    inputs = len(args)
    rows = sum(p[4] for p in pieces)
    outputs = 3 if not last else 2 + len(blocks)

    def body(*refs):
        q_ref = refs[0]
        if not fresh_state:
            m_in, l_in, a_in = refs[first : first + 3]
        outs = refs[inputs : inputs + outputs]
        m_out, l_out = outs[:2]
        s0_ref, s1_ref, p0_ref, p1_ref, vt_ref, fade_ref = refs[inputs + outputs :][:6]
        a_out = refs[-1] if last else outs[2]

        def lanes_of(p):
            return pl.ds(pl.multiple_of(p * LANES, LANES), LANES)

        def score(p, side):
            kk = jnp.concatenate([refs[i][at, lanes_of(p)] for i, at, _, _ in spots], axis=0)
            qq = q_ref[:, lanes_of(p)]
            lane = lax.broadcasted_iota(jnp.int32, qq.shape, 1)
            mine = (lane < HD) if side == 0 else (lane >= HD)
            qm = jnp.where(mine, qq, jnp.zeros_like(qq))
            return lax.dot_general(
                kk, qm, (((1,), (1,)), ((), ())), preferred_element_type=jnp.float32
            )

        def softmax(h, s_ref, p_ref):
            row = pl.ds(h, 1)
            peak = s_ref[0:8, :]
            for at in range(8, rows, 8):
                peak = jnp.maximum(peak, s_ref[at : at + 8, :])
            peak = jnp.max(peak, axis=0, keepdims=True)
            if not fresh_state:
                old = m_in[row, :]
                peak = jnp.maximum(old, peak)
                fade_ref[row, :] = jnp.exp2((old - peak) * factor)
            m_out[row, :] = peak
            for at in range(0, rows, 16):
                part = s_ref[at : at + 16, :]
                p_ref[at : at + 16, :] = jnp.exp2((part - peak) * factor).astype(jnp.bfloat16)

        def values(h, expo, vt):
            vs = jnp.concatenate([vt, jnp.ones((16, rows), vt.dtype)], axis=0)
            pv = jnp.dot(vs, expo, preferred_element_type=jnp.float32)
            acc = pv[:HD, :]
            total = pv[HD : HD + 1, :]
            row = pl.ds(h, 1)
            arows = pl.ds(pl.multiple_of(h * HD, HD), HD)
            if not fresh_state:
                fade = fade_ref[row, :]
                acc = a_in[arows, :] * fade + acc
                total = l_in[row, :] * fade + total
            l_out[row, :] = total
            a_out[arows, :] = acc / total if last else acc

        def pair_step(p, carry):
            h = 2 * p
            vv = jnp.concatenate([refs[i][at, lanes_of(p)] for _, _, i, at in spots], axis=0)
            vt = vv.T
            s1_ref[...] = score(p, 1)
            softmax(h, s0_ref, p0_ref)
            values(jnp.where(p == 0, heads, h - 1), p1_ref[...], vt_ref[...])
            s0_ref[...] = score(jnp.minimum(p + 1, pairs - 1), 0)
            softmax(h + 1, s1_ref, p1_ref)
            values(h, p0_ref[...], vt[:HD, :])
            vt_ref[...] = vt[HD:, :]
            return carry

        s0_ref[...] = score(0, 0)
        lax.fori_loop(0, pairs, pair_step, 0)
        values(heads - 1, p1_ref[...], vt_ref[...])
        if last:
            dead = lax.broadcasted_iota(jnp.int32, m_out.shape, 0) >= heads
            m_out[...] = jnp.where(dead, 1.0, m_out[...])
            l_out[...] = jnp.where(dead, 1.0, l_out[...])

            def write(lanes, array):
                at = 0
                for o_ref, size in zip(outs[2:], blocks):
                    o_ref[:, lanes] = array[at : at + size, :]
                    at += size

            for p in range(pairs):
                lanes = slice(p * LANES, (p + 1) * LANES)
                write(lanes, a_out[lanes, :].T.astype(jnp.bfloat16))
            parts = [*split_three(m_out[...]), *split_three(l_out[...])]
            parts.append(jnp.zeros((LANES - 6 * hrows, count), jnp.float32))
            stats = jnp.concatenate(parts, axis=0).T.astype(jnp.bfloat16)
            write(slice(features, features + LANES), stats)

    stat = jax.ShapeDtypeStruct((hrows, count), jnp.float32)
    aliases = {}
    if last:
        wide = features + LANES
        outs = (stat, stat) + tuple(jax.ShapeDtypeStruct((n, wide), jnp.bfloat16) for n in blocks)
    else:
        outs = (stat, stat, jax.ShapeDtypeStruct((features + HD, count), jnp.float32))
        if not fresh_state:
            aliases = {first: 0, first + 1: 1, first + 2: 2}
    scratch = [
        pltpu.VMEM((rows, count), jnp.float32),
        pltpu.VMEM((rows, count), jnp.float32),
        pltpu.VMEM((rows, count), jnp.bfloat16),
        pltpu.VMEM((rows, count), jnp.bfloat16),
        pltpu.VMEM((HD, rows), jnp.bfloat16),
        pltpu.VMEM((hrows, count), jnp.float32),
    ]
    if last:
        scratch.append(pltpu.VMEM((features + HD, count), jnp.float32))
    vmem = pl.BlockSpec(memory_space=pltpu.VMEM)
    return pl.pallas_call(
        body,
        out_shape=outs,
        in_specs=[vmem] * inputs,
        out_specs=tuple([vmem] * outputs),
        input_output_aliases=aliases,
        scratch_shapes=scratch,
        cost_estimate=pl.CostEstimate(
            flops=4 * rows * count * features,
            transcendentals=rows * count * heads,
            bytes_accessed=4 * count * features,
        ),
        compiler_params=pltpu.CompilerParams(vmem_limit_bytes=16 * 2**20),
        name="attend",
    )(*args)


def merge_project(parts, weight):
    items, wide = parts[0].shape
    features = wide - LANES
    heads = features // HD
    hrows = round_up(heads + 1, 8)
    width = weight.shape[1]
    factor = (1.0 / math.sqrt(HD)) * math.log2(math.e)

    def body(*refs):
        w_ref, o_ref = refs[-2], refs[-1]
        stats = [r[:, features:].astype(jnp.float32) for r in refs[:-2]]

        def stat(x, which):
            at = 3 * which * hrows
            return (
                x[:, at : at + hrows]
                + x[:, at + hrows : at + 2 * hrows]
                + x[:, at + 2 * hrows : at + 3 * hrows]
            )

        peaks = [stat(x, 0) for x in stats]
        best = peaks[0]
        for m in peaks[1:]:
            best = jnp.maximum(best, m)
        shares = [jnp.exp2((m - best) * factor) * stat(x, 1) for m, x in zip(peaks, stats)]
        total = shares[0]
        for w in shares[1:]:
            total = total + w
        shares = [w / total for w in shares]
        lane = lax.broadcasted_iota(jnp.int32, (items, LANES), 1)
        columns = []
        for p in range(features // LANES):
            joined = jnp.zeros((items, LANES), jnp.float32)
            for r, w in zip(refs[:-2], shares):
                scale = jnp.where(lane < HD, w[:, 2 * p : 2 * p + 1], w[:, 2 * p + 1 : 2 * p + 2])
                joined += r[:, p * LANES : (p + 1) * LANES].astype(jnp.float32) * scale
            columns.append(joined.astype(jnp.bfloat16))
        attn = jnp.concatenate(columns, axis=1)
        out = jnp.dot(attn, w_ref[...], preferred_element_type=jnp.float32)
        o_ref[...] = out.astype(jnp.bfloat16)

    vmem = pl.BlockSpec(memory_space=pltpu.VMEM)
    return pl.pallas_call(
        body,
        out_shape=jax.ShapeDtypeStruct((items, width), jnp.bfloat16),
        in_specs=[vmem] * (len(parts) + 1),
        out_specs=vmem,
        cost_estimate=pl.CostEstimate(
            flops=2 * items * features * width,
            transcendentals=0,
            bytes_accessed=2 * features * width,
        ),
        compiler_params=pltpu.CompilerParams(vmem_limit_bytes=16 * 2**20),
        name="merge_project",
    )(*parts, weight)


def per_device(query, key, value, out_weight):
    rows, features = query.shape
    blks = lax.axis_size("blk")
    nodes = lax.axis_size("node")
    half = blks // 2

    def piece(both):
        return (both, 0, both, rows, rows)

    up = down = None
    held = [(key, 0, value, 0, rows)]
    state = None
    for turn in range(1, half + 1):
        final = turn == half
        if turn > 1:
            up, down = lax.optimization_barrier((up, down))
            held = held[: len(held) - 2] + [piece(up), piece(down)]
        if final:
            k = shifted(up[:rows], "blk", 1)
            v = shifted(down[rows:], "blk", -1)
            arrived = [(k, 0, v, 0, rows)]
        elif turn == 1:
            k_up, k_down = shifted(key, "blk", 1), shifted(key, "blk", -1)
            v_up, v_down = shifted(value, "blk", 1), shifted(value, "blk", -1)
            up = jnp.concatenate([k_up, v_up], axis=0)
            down = jnp.concatenate([k_down, v_down], axis=0)
        else:
            up = shifted(up, "blk", 1)
            down = shifted(down, "blk", -1)
        if not final:
            arrived = [piece(up), piece(down)]
        if turn == 1:
            turns = sorted(range(1, nodes), key=lambda d: -min(d, nodes - d))
            others = {d: shifted(query, "node", d) for d in turns}
            stack = [query] + [others[d] for d in range(1, nodes)]
            blocks = [rows] * nodes
            padded = round_up(rows * nodes, LANES)
            if padded > rows * nodes:
                stack.append(jnp.zeros((padded - rows * nodes, features), query.dtype))
            queries = jnp.concatenate(stack, axis=0)
        else:
            state = attend_step(queries, held, state, False)
            held = []
        held = held + arrived

    parts = list(attend_step(queries, held, state, True, blocks)[2:])
    for d in turns:
        parts[d] = shifted(parts[d], "node", -d)
    mine = merge_project(parts, out_weight)

    cores = lax.axis_size("pair")
    at = lax.axis_index("pair")
    tiles = mine.reshape(cores, rows // cores, mine.shape[1])
    summed = lax.dynamic_index_in_dim(tiles, at, 0, keepdims=False).astype(jnp.float32)
    for d in range(1, cores):
        away = lax.dynamic_index_in_dim(tiles, (at + d) % cores, 0, keepdims=False)
        summed = summed + shifted(away, "pair", d).astype(jnp.float32)
    return summed.astype(jnp.bfloat16)


def solution(mesh):
    in_specs = (
        P(("grp", "blk", "node"), "pair"),
        P(("grp", "blk", "node"), "pair"),
        P(("grp", "blk", "node"), "pair"),
        P("pair", None),
    )
    out_specs = P(("grp", "blk", "node", "pair"), None)

    return jax.shard_map(
        per_device, mesh=mesh, in_specs=in_specs, out_specs=out_specs, check_vma=False
    )
```

```python
import math

import jax
import jax.numpy as jnp
from jax import lax
from jax.experimental import pallas as pl
from jax.experimental.pallas import tpu as pltpu
from jax.sharding import PartitionSpec as P


HD = 64
LANES = 128


def round_up(value, unit):
    return -(-value // unit) * unit


def shifted(array, axis, by):
    size = lax.axis_size(axis)
    return lax.ppermute(array, axis, [(i, (i + by) % size) for i in range(size)])


def split_three(x):
    hi = x.astype(jnp.bfloat16).astype(jnp.float32)
    rest = x - hi
    mid = rest.astype(jnp.bfloat16).astype(jnp.float32)
    return hi, mid, rest - mid


def attend_step(queries, pieces, state, last, blocks=None):
    count, features = queries.shape
    pairs = features // LANES
    heads = features // HD
    hrows = round_up(heads + 1, 8)
    factor = (1.0 / math.sqrt(HD)) * math.log2(math.e)
    fresh_state = state is None

    args = [queries]
    spots = []
    for k, k_at, v, v_at, size in pieces:
        args.append(k)
        at = len(args) - 1
        if v is not k:
            args.append(v)
        spots.append((at, slice(k_at, k_at + size), len(args) - 1, slice(v_at, v_at + size)))
    first = len(args)
    if not fresh_state:
        args += list(state)
    inputs = len(args)
    rows = sum(p[4] for p in pieces)
    outputs = 3 if not last else 2 + len(blocks)

    def body(*refs):
        q_ref = refs[0]
        if not fresh_state:
            m_in, l_in, a_in = refs[first : first + 3]
        outs = refs[inputs : inputs + outputs]
        m_out, l_out = outs[:2]
        s0_ref, s1_ref, p0_ref, p1_ref, vt_ref, fade_ref = refs[inputs + outputs :][:6]
        a_out = refs[-1] if last else outs[2]

        def lanes_of(p):
            return pl.ds(pl.multiple_of(p * LANES, LANES), LANES)

        def score(p, side):
            kk = jnp.concatenate([refs[i][at, lanes_of(p)] for i, at, _, _ in spots], axis=0)
            qq = q_ref[:, lanes_of(p)]
            lane = lax.broadcasted_iota(jnp.int32, qq.shape, 1)
            mine = (lane < HD) if side == 0 else (lane >= HD)
            qm = jnp.where(mine, qq, jnp.zeros_like(qq))
            return lax.dot_general(
                kk, qm, (((1,), (1,)), ((), ())), preferred_element_type=jnp.float32
            )

        def softmax(h, s_ref, p_ref):
            row = pl.ds(h, 1)
            peak = s_ref[0:8, :]
            for at in range(8, rows, 8):
                peak = jnp.maximum(peak, s_ref[at : at + 8, :])
            peak = jnp.max(peak, axis=0, keepdims=True)
            if not fresh_state:
                old = m_in[row, :]
                peak = jnp.maximum(old, peak)
                fade_ref[row, :] = jnp.exp2((old - peak) * factor)
            m_out[row, :] = peak
            for at in range(0, rows, 16):
                part = s_ref[at : at + 16, :]
                p_ref[at : at + 16, :] = jnp.exp2((part - peak) * factor).astype(jnp.bfloat16)

        def values(h, expo, vt):
            vs = jnp.concatenate([vt, jnp.ones((16, rows), vt.dtype)], axis=0)
            pv = jnp.dot(vs, expo, preferred_element_type=jnp.float32)
            acc = pv[:HD, :]
            total = pv[HD : HD + 1, :]
            row = pl.ds(h, 1)
            arows = pl.ds(pl.multiple_of(h * HD, HD), HD)
            if not fresh_state:
                fade = fade_ref[row, :]
                acc = a_in[arows, :] * fade + acc
                total = l_in[row, :] * fade + total
            l_out[row, :] = total
            a_out[arows, :] = acc / total if last else acc

        def pair_step(p, carry):
            h = 2 * p
            vv = jnp.concatenate([refs[i][at, lanes_of(p)] for _, _, i, at in spots], axis=0)
            vt = vv.T
            s1_ref[...] = score(p, 1)
            softmax(h, s0_ref, p0_ref)
            values(jnp.where(p == 0, heads, h - 1), p1_ref[...], vt_ref[...])
            s0_ref[...] = score(jnp.minimum(p + 1, pairs - 1), 0)
            softmax(h + 1, s1_ref, p1_ref)
            values(h, p0_ref[...], vt[:HD, :])
            vt_ref[...] = vt[HD:, :]
            return carry

        s0_ref[...] = score(0, 0)
        lax.fori_loop(0, pairs, pair_step, 0)
        values(heads - 1, p1_ref[...], vt_ref[...])
        if last:
            dead = lax.broadcasted_iota(jnp.int32, m_out.shape, 0) >= heads
            m_out[...] = jnp.where(dead, 1.0, m_out[...])
            l_out[...] = jnp.where(dead, 1.0, l_out[...])

            def write(lanes, array):
                at = 0
                for o_ref, size in zip(outs[2:], blocks):
                    o_ref[:, lanes] = array[at : at + size, :]
                    at += size

            for p in range(pairs):
                lanes = slice(p * LANES, (p + 1) * LANES)
                write(lanes, a_out[lanes, :].T.astype(jnp.bfloat16))
            parts = [*split_three(m_out[...]), *split_three(l_out[...])]
            parts.append(jnp.zeros((LANES - 6 * hrows, count), jnp.float32))
            stats = jnp.concatenate(parts, axis=0).T.astype(jnp.bfloat16)
            write(slice(features, features + LANES), stats)

    stat = jax.ShapeDtypeStruct((hrows, count), jnp.float32)
    aliases = {}
    if last:
        wide = features + LANES
        outs = (stat, stat) + tuple(jax.ShapeDtypeStruct((n, wide), jnp.bfloat16) for n in blocks)
    else:
        outs = (stat, stat, jax.ShapeDtypeStruct((features + HD, count), jnp.float32))
        if not fresh_state:
            aliases = {first: 0, first + 1: 1, first + 2: 2}
    scratch = [
        pltpu.VMEM((rows, count), jnp.float32),
        pltpu.VMEM((rows, count), jnp.float32),
        pltpu.VMEM((rows, count), jnp.bfloat16),
        pltpu.VMEM((rows, count), jnp.bfloat16),
        pltpu.VMEM((HD, rows), jnp.bfloat16),
        pltpu.VMEM((hrows, count), jnp.float32),
    ]
    if last:
        scratch.append(pltpu.VMEM((features + HD, count), jnp.float32))
    vmem = pl.BlockSpec(memory_space=pltpu.VMEM)
    return pl.pallas_call(
        body,
        out_shape=outs,
        in_specs=[vmem] * inputs,
        out_specs=tuple([vmem] * outputs),
        input_output_aliases=aliases,
        scratch_shapes=scratch,
        cost_estimate=pl.CostEstimate(
            flops=4 * rows * count * features,
            transcendentals=rows * count * heads,
            bytes_accessed=4 * count * features,
        ),
        compiler_params=pltpu.CompilerParams(vmem_limit_bytes=16 * 2**20),
        name="attend",
    )(*args)


def merge_project(parts, weight):
    items, wide = parts[0].shape
    features = wide - LANES
    heads = features // HD
    hrows = round_up(heads + 1, 8)
    width = weight.shape[1]
    factor = (1.0 / math.sqrt(HD)) * math.log2(math.e)

    def body(*refs):
        w_ref, o_ref = refs[-2], refs[-1]
        stats = [r[:, features:].astype(jnp.float32) for r in refs[:-2]]

        def stat(x, which):
            at = 3 * which * hrows
            return (
                x[:, at : at + hrows]
                + x[:, at + hrows : at + 2 * hrows]
                + x[:, at + 2 * hrows : at + 3 * hrows]
            )

        peaks = [stat(x, 0) for x in stats]
        best = peaks[0]
        for m in peaks[1:]:
            best = jnp.maximum(best, m)
        shares = [jnp.exp2((m - best) * factor) * stat(x, 1) for m, x in zip(peaks, stats)]
        total = shares[0]
        for w in shares[1:]:
            total = total + w
        shares = [w / total for w in shares]
        lane = lax.broadcasted_iota(jnp.int32, (items, LANES), 1)
        columns = []
        for p in range(features // LANES):
            joined = jnp.zeros((items, LANES), jnp.float32)
            for r, w in zip(refs[:-2], shares):
                scale = jnp.where(lane < HD, w[:, 2 * p : 2 * p + 1], w[:, 2 * p + 1 : 2 * p + 2])
                joined += r[:, p * LANES : (p + 1) * LANES].astype(jnp.float32) * scale
            columns.append(joined.astype(jnp.bfloat16))
        attn = jnp.concatenate(columns, axis=1)
        out = jnp.dot(attn, w_ref[...], preferred_element_type=jnp.float32)
        o_ref[...] = out.astype(jnp.bfloat16)

    vmem = pl.BlockSpec(memory_space=pltpu.VMEM)
    return pl.pallas_call(
        body,
        out_shape=jax.ShapeDtypeStruct((items, width), jnp.bfloat16),
        in_specs=[vmem] * (len(parts) + 1),
        out_specs=vmem,
        cost_estimate=pl.CostEstimate(
            flops=2 * items * features * width,
            transcendentals=0,
            bytes_accessed=2 * features * width,
        ),
        compiler_params=pltpu.CompilerParams(vmem_limit_bytes=16 * 2**20),
        name="merge_project",
    )(*parts, weight)


def per_device(query, key, value, out_weight):
    rows, features = query.shape
    blks = lax.axis_size("blk")
    nodes = lax.axis_size("node")
    half = blks // 2

    def piece(both):
        return (both, 0, both, rows, rows)

    up = down = None
    held = [(key, 0, value, 0, rows)]
    state = None
    for turn in range(1, half + 1):
        final = turn == half
        if final:
            k = shifted(up[:rows], "blk", 1)
            v = shifted(down[rows:], "blk", -1)
            arrived = [(k, 0, v, 0, rows)]
        elif turn == 1:
            k_up, k_down = shifted(key, "blk", 1), shifted(key, "blk", -1)
            v_up, v_down = shifted(value, "blk", 1), shifted(value, "blk", -1)
            up = jnp.concatenate([k_up, v_up], axis=0)
            down = jnp.concatenate([k_down, v_down], axis=0)
        else:
            up = shifted(up, "blk", 1)
            down = shifted(down, "blk", -1)
        if not final:
            arrived = [piece(up), piece(down)]
        if turn == 1:
            turns = sorted(range(1, nodes), key=lambda d: -min(d, nodes - d))
            others = {d: shifted(query, "node", d) for d in turns}
            stack = [query] + [others[d] for d in range(1, nodes)]
            blocks = [rows] * nodes
            padded = round_up(rows * nodes, LANES)
            if padded > rows * nodes:
                stack.append(jnp.zeros((padded - rows * nodes, features), query.dtype))
            queries = jnp.concatenate(stack, axis=0)
        else:
            state = attend_step(queries, held, state, False)
            held = []
        held = held + arrived

    parts = list(attend_step(queries, held, state, True, blocks)[2:])
    for d in reversed(turns):
        parts[d] = shifted(parts[d], "node", -d)
    mine = merge_project(parts, out_weight)

    cores = lax.axis_size("pair")
    at = lax.axis_index("pair")
    tiles = mine.reshape(cores, rows // cores, mine.shape[1])
    summed = lax.dynamic_index_in_dim(tiles, at, 0, keepdims=False).astype(jnp.float32)
    for d in range(1, cores):
        away = lax.dynamic_index_in_dim(tiles, (at + d) % cores, 0, keepdims=False)
        summed = summed + shifted(away, "pair", d).astype(jnp.float32)
    return summed.astype(jnp.bfloat16)


def solution(mesh):
    in_specs = (
        P(("grp", "blk", "node"), "pair"),
        P(("grp", "blk", "node"), "pair"),
        P(("grp", "blk", "node"), "pair"),
        P("pair", None),
    )
    out_specs = P(("grp", "blk", "node", "pair"), None)

    return jax.shard_map(
        per_device, mesh=mesh, in_specs=in_specs, out_specs=out_specs, check_vma=False
    )
```
